128 devices in a mesh: gx: 16 (over y, x), gy: 8 (over z, core).
Axes of the slice: x: 4, y: 4, z: 4, core: 2. Of those that a mesh axis runs over, the one named last changes fastest.
Arguments:
- source_field: bfloat16 [16384, 128, 128], P(('gx', 'gy')), may hold values from -6 to 6
- weight_blocks: bfloat16 [65536, 128, 128], P(('gx', 'gy')), may hold values from -0.1875 to 0.1875
- source_ids: int32 [65536], replicated, may hold values from 0 to 16383, as said below
- target_ids: int32 [65536], replicated, may hold values from 0 to 8191, as said below
Outputs:
- remapped: bfloat16 [8192, 128, 128], P(('gx', 'gy'))
The draws below stay inside these ranges and needn't reach their ends.
Inputs may be any that keep to these rules, and one draw needn't show every extreme that they name: `source_ids`: source block b lies on device b // 128 of gx+gy, and weight block k lies on device k // 512. The weight blocks of device d name only source blocks of devices d - 2 to d + 2. Among the weight blocks of one device, at most 64 distinct source blocks of any one other device are named, and exactly 64 for some other device. `target_ids`: target block t lies on device t // 64 of gx+gy. The weight blocks of device d name only target blocks of devices d - 2 to d + 2. Among the weight blocks of one device, at most 16 distinct target blocks of any one device are named, and exactly 16 for some other device.
All inputs are finite; a program needn't handle non-finite values.
Results may differ from the reference program's by a relative error of at most 0.001.
Values may be sent and summed in bfloat16 or wider, within the bound.
A program may use at most 192 MiB of HBM per device.

```python
import jax
import jax.numpy as jnp
from jax import lax

BLK = 128
CH = 128
HALF = 2
SB_DEV = 128
TB_DEV = 64
WB_DEV = 512
CAP_S = 64
CAP_T = 16
NSB = 16384
NW = 65536
N_GX = 16
N_GY = 8


def pair_ids(key, slot_count, per_device):
    devices = N_GX * N_GY
    span = 2 * HALF + 1

    def one_device(device):
        keyed = jax.random.fold_in(key, device)
        key_count, key_force, key_perm, key_pick, key_order = jax.random.split(keyed, 5)
        offsets = jnp.arange(span, dtype=jnp.int32) - HALF
        owner = device + offsets
        valid = (owner >= 0) & (owner < devices)
        counts = jax.random.randint(key_count, (span,), slot_count // 2, slot_count + 1)
        scores = jax.random.randint(key_force, (span,), 0, 1024) * span + jnp.arange(span, dtype=jnp.int32)
        scores = jnp.where(valid & (offsets != 0), scores, -1)
        forced = jnp.argmax(scores)
        counts = jnp.where((jnp.arange(span, dtype=jnp.int32) == forced) | (offsets == 0), slot_count, counts)
        counts = jnp.where(valid, counts, 0)
        perms = jax.vmap(lambda kk: jax.random.permutation(kk, per_device))(jax.random.split(key_perm, span))
        chosen = perms[:, :slot_count].reshape(-1)
        used = (jnp.arange(slot_count, dtype=jnp.int32)[None, :] < counts[:, None]).reshape(-1)
        entries = span * slot_count
        block_index = jnp.arange(WB_DEV, dtype=jnp.int32)
        picked = jax.random.randint(key_pick, (WB_DEV,), 0, entries)
        entry = jnp.where(block_index < entries, block_index, picked)
        entry = jnp.where(used[entry], entry, HALF * slot_count + entry % slot_count)
        order = jax.random.permutation(key_order, WB_DEV)
        entry = entry[order]
        return (owner[entry // slot_count] * per_device + chosen[entry]).astype(jnp.int32)
    return jax.vmap(one_device)(jnp.arange(devices, dtype=jnp.int32)).reshape(-1).astype(jnp.int32)


def draw_source_ids(key, part):
    return pair_ids(jax.random.fold_in(key, 11), CAP_S, SB_DEV)


def draw_target_ids(key, part):
    return pair_ids(jax.random.fold_in(key, 23), CAP_T, TB_DEV)


def shard_levels(stream_key, shape, pieces, least, largest):
    gain = 1.0
    for dim, parts in pieces:
        draws = jax.random.uniform(jax.random.fold_in(jax.random.fold_in(stream_key, 6), dim), (parts,), jnp.float32, least / len(pieces), largest / len(pieces))
        gain = gain * jnp.repeat(jnp.exp(draws), shape[dim] // parts).reshape((-1,) + (1,) * (len(shape) - 1 - dim))
    return gain


def centred(own_key, shape, scale, most, cuts=(), kind=jnp.bfloat16):
    gain = shard_levels(own_key, shape, cuts, -0.22, 0.18) if cuts else 1.0
    array = jax.random.normal(own_key, shape, jnp.float32) * scale * gain
    return jnp.minimum(jnp.maximum(array, -most), most).astype(kind)


def setup_inputs(seed: int = 0) -> dict:
    splits = jax.random.split(jax.random.key(seed), 5)
    return {
        "source_field": centred(splits[0], (NSB, BLK, CH), 1.0, 6.0, ((0, 128),)),
        "weight_blocks": centred(splits[1], (NW, BLK, BLK), (BLK * WB_DEV // TB_DEV) ** -0.5, 0.1875, ((0, 128),)),
        "source_ids": draw_source_ids(jax.random.fold_in(splits[4], 71), 0),
        "target_ids": draw_target_ids(jax.random.fold_in(splits[4], 71), 0),
    }


def reference(source_field, weight_blocks, source_ids, target_ids):
    devices = N_GX * N_GY
    total = jnp.zeros((TB_DEV * devices, BLK, CH), jnp.float32)

    def accumulate(carry, index):
        start = (index * WB_DEV).astype(jnp.int32)
        weights = lax.dynamic_slice_in_dim(weight_blocks, start, WB_DEV, 0)
        src_rows = lax.dynamic_slice_in_dim(source_ids, start, WB_DEV, 0)
        tgt_rows = lax.dynamic_slice_in_dim(target_ids, start, WB_DEV, 0)
        gathered = source_field[src_rows]
        partial_value = jnp.einsum("kts,ksc->ktc", weights.astype(jnp.float32), gathered.astype(jnp.float32))
        return carry.at[tgt_rows].add(partial_value), None

    total, _ = lax.scan(accumulate, total, jnp.arange(devices, dtype=jnp.int32))
    return total.astype(jnp.bfloat16)
```

```python
import functools

import jax
import jax.numpy as jnp
from jax import lax
from jax.experimental import pallas as pl
from jax.experimental.pallas import tpu as pltpu
from jax.sharding import PartitionSpec as P

BLK = 128
SB = 128
TB = 64
WB = 512
CS = 64
CT = 16
AXES = ("gx", "gy")
TRASH = 80
SLOTS = 84
GROUP = 8
RING = 32
CAP = WB + 2 * GROUP
QROWS = CT * BLK + 16


f32 = jnp.float32
i32 = jnp.int32
bf16 = jnp.bfloat16


def iota(dim):
    return lax.broadcasted_iota(i32, (BLK, BLK), dim)


def presence(rows, base, limit):
    sub = iota(0)
    hits = jnp.zeros((BLK, BLK), f32)
    for q in range(4):
        hits = hits + (jnp.broadcast_to(rows[q : q + 1, :] - base, (BLK, BLK)) == sub).astype(f32)
    count = jnp.dot(hits.astype(bf16), jnp.ones((BLK, BLK), bf16), preferred_element_type=f32)
    return ((count > 0.5) & (sub < limit)).astype(f32)


def ranks(present):
    lower = (iota(1) < iota(0)).astype(bf16)
    return jnp.dot(lower, present.astype(bf16), preferred_element_type=f32)


def listed(present, rank, fill):
    sel = (present > 0.5) & (rank == iota(1).astype(f32))
    found = jnp.sum(sel.astype(f32), axis=0, keepdims=True)
    index = jnp.sum(jnp.where(sel, iota(0).astype(f32), 0.0), axis=0, keepdims=True)
    return jnp.where(found > 0.5, index, fill).astype(i32)


def ranked(rows, base, rank):
    out = []
    for q in range(4):
        sel = jnp.broadcast_to(rows[q : q + 1, :] - base, (BLK, BLK)) == iota(0)
        out.append(jnp.sum(jnp.where(sel, rank, 0.0), axis=0, keepdims=True))
    return jnp.concatenate(out, axis=0).astype(i32)


def pack_kernel(n, sids, tids, src, p2m, p2p, pn, pd, enc, recv, sid_v, tid_v, src_v, list_v, list_s, sems, fsem):
    me = lax.axis_index(AXES)
    odd = me % 2
    part = 1 - 2 * odd
    cross = -part
    fetch = pltpu.make_async_copy(src, src_v, sems.at[10])
    fetch.start()
    loads = []
    for r in range(5):
        e = jnp.clip(me + (r - 2), 0, n - 1)
        loads.append(pltpu.make_async_copy(sids.at[e], sid_v.at[r], sems.at[r]))
        loads.append(pltpu.make_async_copy(tids.at[e], tid_v.at[r], sems.at[5 + r]))
    for c in loads:
        c.start()
    for c in loads:
        c.wait()
    rels = (-2, 2, part, cross)
    for f, rel in enumerate(rels):
        present = presence(sid_v[2 + rel], me * SB, SB)
        list_v[f : f + 1, :] = listed(present, ranks(present), 0.0)
    move = pltpu.make_async_copy(list_v, list_s, sems.at[11])
    move.start()

    own = sid_v[2]
    rel_of = (own // SB) - me
    pos = own - me * SB
    stage = jnp.zeros((4, BLK), i32)
    for f, rel in enumerate((-2, 2, part, cross)):
        base = (me + rel) * SB
        rank = ranked(own, base, ranks(presence(own, base, SB)))
        here = rel_of == rel
        pos = jnp.where(here, rank + (0 if f == 3 else f * CS), pos)
        stage = jnp.where(here, 2 if f == 3 else 1, stage)
    town = tid_v[2]
    trel = town // TB - me
    slot = jnp.zeros((4, BLK), i32)
    for f, rel in enumerate((0, -2, 2, part, cross)):
        base = (me + rel) * TB
        rank = ranked(town, base, ranks(presence(town, base, TB)))
        slot = jnp.where(trel == rel, rank + f * CT, slot)
    k = lax.broadcasted_iota(i32, (4, BLK), 0) * BLK + lax.broadcasted_iota(i32, (4, BLK), 1)
    enc[...] = k + pos * 512 + slot * (1 << 17) + stage * (1 << 24)
    for f, rel in enumerate((0, 2, -2, part, cross)):
        present = presence(tid_v[2 + rel], me * TB, TB)
        e = me + rel
        present = jnp.where((e >= 0) & (e < n), present, 0.0)
        recv[f : f + 1, :] = listed(present, ranks(present), float(TB))

    move.wait()
    fetch.wait()
    outs = (p2m, p2p, pd, pn)
    for f in (0, 1, 3, 2):

        def send(r, carry, f=f):
            for u in range(4):
                b = list_s[f, r * 4 + u]
                pltpu.make_async_copy(src_v.at[b], outs[f].at[r * 4 + u], fsem.at[f]).start()
            return carry

        lax.fori_loop(0, CS // 4, send, 0)
    for f in (0, 1, 3, 2):
        pltpu.make_async_copy(src_v.at[pl.ds(0, CS)], outs[f], fsem.at[f]).wait()


def call_pack(n, sids, tids, src):
    flow = jax.ShapeDtypeStruct((CS, BLK, BLK), bf16)
    any_ = pl.BlockSpec(memory_space=pl.ANY)
    vm = pl.BlockSpec(memory_space=pltpu.VMEM)
    return pl.pallas_call(
        functools.partial(pack_kernel, n),
        out_shape=[flow] * 4 + [jax.ShapeDtypeStruct((4, BLK), i32), jax.ShapeDtypeStruct((8, BLK), i32)],
        in_specs=[any_] * 3,
        out_specs=[any_] * 4 + [vm, vm],
        scratch_shapes=[
            pltpu.VMEM((5, 4, BLK), i32),
            pltpu.VMEM((5, 4, BLK), i32),
            pltpu.VMEM((SB, BLK, BLK), bf16),
            pltpu.VMEM((8, BLK), i32),
            pltpu.SMEM((8, BLK), i32),
            pltpu.SemaphoreType.DMA((12,)),
            pltpu.SemaphoreType.DMA((4,)),
        ],
        name="pack",
        cost_estimate=pl.CostEstimate(flops=100_000_000, bytes_accessed=12_600_000, transcendentals=0),
    )(sids, tids, src)


def products(lists, base, count, w, tab, acc, wbuf, wsem):
    groups = (count + GROUP - 1) // GROUP

    def fetch(i, slot):
        k = lists[base + i] & 511
        pltpu.make_async_copy(w.at[k], wbuf.at[slot], wsem.at[slot]).start()

    for g in range(RING // GROUP):

        @pl.when(g < groups)
        def _():
            for u in range(GROUP):
                fetch(g * GROUP + u, g * GROUP + u)

    def step(g, carry):
        ring = lax.rem(g, RING // GROUP) * GROUP
        parts = []
        slots = []
        for u in range(GROUP):
            entry = lists[base + g * GROUP + u]
            pltpu.make_async_copy(w.at[0], wbuf.at[ring + u], wsem.at[ring + u]).wait()
            pos = (entry >> 9) & 255
            slots.append((entry >> 17) & 127)
            parts.append(jnp.dot(wbuf[ring + u], tab[pos], preferred_element_type=f32))
        for u in range(GROUP):
            acc[slots[u]] = acc[slots[u]] + parts[u]

        @pl.when(g + RING // GROUP < groups)
        def _():
            for u in range(GROUP):
                fetch((g + RING // GROUP) * GROUP + u, ring + u)

        return carry

    lax.fori_loop(0, groups, step, 0)


def first_kernel(enc, w, src, acc_out, lists, counts, tab, acc, wbuf, wsem, sems):
    fetch = pltpu.make_async_copy(src, tab, sems.at[0])
    fetch.start()

    def clear(i, carry):
        acc[i] = jnp.zeros((BLK, BLK), f32)
        return carry

    lax.fori_loop(0, SLOTS, clear, 0)
    for s in range(3):
        counts[s] = 0

    def place(i, carry):
        for u in range(4):
            v = enc[i // 32, (i % 32) * 4 + u]
            s = v >> 24
            c = counts[s]
            lists[s * CAP + c] = v
            counts[s] = c + 1
        return carry

    lax.fori_loop(0, WB // 4, place, 0)
    for s in range(3):
        for u in range(GROUP):
            lists[s * CAP + counts[s] + u] = TRASH << 17
    fetch.wait()
    products(lists, 0, counts[0], w, tab, acc, wbuf, wsem)
    out = pltpu.make_async_copy(acc, acc_out, sems.at[1])
    out.start()
    out.wait()


def work_scratch(blocks):
    return [
        pltpu.VMEM((blocks, BLK, BLK), bf16),
        pltpu.VMEM((SLOTS, BLK, BLK), f32),
        pltpu.VMEM((RING, BLK, BLK), bf16),
        pltpu.SemaphoreType.DMA((RING,)),
        pltpu.SemaphoreType.DMA((8,)),
    ]


def cost(blocks):
    return pl.CostEstimate(flops=blocks * 2 * BLK**3, bytes_accessed=blocks * 64 * 1024, transcendentals=0)


any_spec = pl.BlockSpec(memory_space=pl.ANY)
sm_spec = pl.BlockSpec(memory_space=pltpu.SMEM)
acc_shape = jax.ShapeDtypeStruct((SLOTS, BLK, BLK), f32)


def call_first(enc, w, src):
    return pl.pallas_call(
        first_kernel,
        out_shape=[acc_shape, jax.ShapeDtypeStruct((3 * CAP,), i32), jax.ShapeDtypeStruct((8,), i32)],
        in_specs=[sm_spec, any_spec, any_spec],
        out_specs=[any_spec, sm_spec, sm_spec],
        scratch_shapes=work_scratch(SB),
        name="own",
        cost_estimate=cost(512),
    )(enc, w, src)


def second_kernel(lists, counts, w, a, b, c, acc_in, acc_out, tab, acc, wbuf, wsem, sems):
    loads = [pltpu.make_async_copy(acc_in, acc, sems.at[0])]
    for i, r in enumerate((a, b, c)):
        loads.append(pltpu.make_async_copy(r, tab.at[pl.ds(i * CS, CS)], sems.at[1 + i]))
    for x in loads:
        x.start()
    for x in loads:
        x.wait()
    products(lists, CAP, counts[1], w, tab, acc, wbuf, wsem)
    out = pltpu.make_async_copy(acc, acc_out, sems.at[4])
    out.start()
    out.wait()


def call_second(lists, counts, w, a, b, c, acc):
    return pl.pallas_call(
        second_kernel,
        out_shape=acc_shape,
        in_specs=[sm_spec, sm_spec] + [any_spec] * 5,
        out_specs=any_spec,
        scratch_shapes=work_scratch(3 * CS),
        name="mid",
        cost_estimate=cost(512),
    )(lists, counts, w, a, b, c, acc)


def third_kernel(lists, counts, w, a, acc_in, own, q2m, q2p, qd, qn, tab, acc, wbuf, wsem, sems, qbuf, qsem):
    loads = [pltpu.make_async_copy(acc_in, acc, sems.at[0]), pltpu.make_async_copy(a, tab, sems.at[1])]
    for x in loads:
        x.start()
    for x in loads:
        x.wait()
    products(lists, 2 * CAP, counts[2], w, tab, acc, wbuf, wsem)
    mine = pltpu.make_async_copy(acc.at[pl.ds(0, CT)], own, sems.at[2])
    mine.start()
    outs = (q2m, q2p, qd, qn)
    sends = []
    for f in (0, 1, 3, 2):

        def quantize(s, carry, f=f):
            x = acc[CT + f * CT + s]
            top = jnp.max(jnp.abs(x), axis=0, keepdims=True)
            e = jnp.ceil(jnp.log2(jnp.maximum(top, 1e-30)))
            q = jnp.clip(jnp.round(x * jnp.exp2(15.0 - e)), -32767.0, 32767.0)
            row = pl.multiple_of(s * BLK, BLK)
            qbuf[f, pl.ds(row, BLK), :] = q.astype(i32).astype(jnp.int16)
            return jnp.where(lax.broadcasted_iota(i32, (CT, BLK), 0) == s, e.astype(i32), carry)

        exps = lax.fori_loop(0, CT, quantize, jnp.zeros((CT, BLK), i32))
        qbuf[f, pl.ds(CT * BLK, CT), :] = exps.astype(jnp.int16)
        sends.append(pltpu.make_async_copy(qbuf.at[f], outs[f], qsem.at[f]))
        sends[-1].start()
    for x in sends:
        x.wait()
    mine.wait()


def call_third(lists, counts, w, a, acc):
    q = jax.ShapeDtypeStruct((QROWS, BLK), jnp.int16)
    return pl.pallas_call(
        third_kernel,
        out_shape=[jax.ShapeDtypeStruct((CT, BLK, BLK), f32)] + [q] * 4,
        in_specs=[sm_spec, sm_spec] + [any_spec] * 3,
        out_specs=[any_spec] * 5,
        scratch_shapes=work_scratch(CS) + [pltpu.VMEM((4, QROWS, BLK), jnp.int16), pltpu.SemaphoreType.DMA((4,))],
        name="last",
        cost_estimate=cost(256),
    )(lists, counts, w, a, acc)


def final_kernel(recv, own, a, b, c, d, out, total, own_v, q_v, sems):
    loads = [pltpu.make_async_copy(own, own_v, sems.at[0])]
    for i, r in enumerate((a, b, c, d)):
        loads.append(pltpu.make_async_copy(r, q_v.at[i], sems.at[1 + i]))
    for x in loads:
        x.start()

    def clear(i, carry):
        total[i] = jnp.zeros((BLK, BLK), f32)
        return carry

    lax.fori_loop(0, TB, clear, 0)
    loads[0].wait()

    def add_own(r, carry):
        t = recv[0, r]
        total[t] = total[t] + own_v[r]
        return carry

    lax.fori_loop(0, CT, add_own, 0)
    for f in range(4):
        loads[1 + f].wait()
        exps = q_v[f, pl.ds(CT * BLK, CT), :].astype(f32)
        scale = jnp.exp2(exps - 15.0)
        for r in range(CT):
            t = recv[1 + f, r]
            q = q_v[f, pl.ds(r * BLK, BLK), :].astype(f32)
            total[t] = total[t] + q * scale[r : r + 1, :]

    def store(i, carry):
        out[i] = total[i].astype(bf16)
        return carry

    lax.fori_loop(0, TB, store, 0)


def call_final(recv, own, a, b, c, d):
    return pl.pallas_call(
        final_kernel,
        out_shape=jax.ShapeDtypeStruct((TB, BLK, BLK), bf16),
        in_specs=[sm_spec] + [any_spec] * 5,
        out_specs=pl.BlockSpec(memory_space=pltpu.VMEM),
        scratch_shapes=[
            pltpu.VMEM((TB + 1, BLK, BLK), f32),
            pltpu.VMEM((CT, BLK, BLK), f32),
            pltpu.VMEM((4, QROWS, BLK), jnp.int16),
            pltpu.SemaphoreType.DMA((5,)),
        ],
        name="final",
        cost_estimate=cost(64),
    )(recv, own, a, b, c, d)


def swaps(n):
    partner = [(d, d ^ 1) for d in range(n)]
    across = [(d, d + 1 if d % 2 else d - 1) for d in range(1, n - 1)]
    up = [(d, d + 2) for d in range(n - 2)]
    down = [(d, d - 2) for d in range(2, n)]
    return down, up, partner, across


def body(source_field, weight_blocks, source_ids, target_ids):
    n = lax.axis_size(AXES)
    down, up, partner, across = swaps(n)
    p2m, p2p, pn, pd, enc, recv = call_pack(
        n, source_ids.reshape(n, 4, BLK), target_ids.reshape(n, 4, BLK), source_field
    )
    send = lambda x, pairs: lax.ppermute(x, AXES, pairs)
    from_up = send(p2m, down)
    from_down = send(p2p, up)
    from_cross = send(pn, across)
    from_part = send(pd, partner)
    acc, lists, counts = call_first(enc, weight_blocks, source_field)
    acc = call_second(lists, counts, weight_blocks, from_down, from_up, from_part, acc)
    own, q2m, q2p, qd, qn = call_third(lists, counts, weight_blocks, from_cross, acc)
    a = send(q2m, down)
    b = send(q2p, up)
    d = send(qn, across)
    c = send(qd, partner)
    return call_final(recv, own, a, b, c, d)


def solution(mesh):
    return jax.shard_map(
        body,
        mesh=mesh,
        in_specs=(P(AXES, None, None), P(AXES, None, None), P(), P()),
        out_specs=P(AXES, None, None),
        check_vma=False,
    )
```

```python
import functools

import jax
import jax.numpy as jnp
from jax import lax
from jax.experimental import pallas as pl
from jax.experimental.pallas import tpu as pltpu
from jax.sharding import PartitionSpec as P

BLK = 128
SB = 128
TB = 64
WB = 512
CS = 64
CT = 16
AXES = ("gx", "gy")
TRASH = 80
SLOTS = 84
GROUP = 16
VLIM = 9 * 1024 * 1024
HALF_ROWS = CT // 2 * BLK + 16


f32 = jnp.float32
i32 = jnp.int32
bf16 = jnp.bfloat16


def iota(dim):
    return lax.broadcasted_iota(i32, (BLK, BLK), dim)


def presence(rows, base, limit):
    sub = iota(0)
    hits = jnp.zeros((BLK, BLK), f32)
    for q in range(4):
        hits = hits + (jnp.broadcast_to(rows[q : q + 1, :] - base, (BLK, BLK)) == sub).astype(f32)
    count = jnp.dot(hits.astype(bf16), jnp.ones((BLK, BLK), bf16), preferred_element_type=f32)
    return ((count > 0.5) & (sub < limit)).astype(f32)


def ranks(present):
    lower = (iota(1) < iota(0)).astype(bf16)
    return jnp.dot(lower, present.astype(bf16), preferred_element_type=f32)


def listed(present, rank, fill):
    sel = (present > 0.5) & (rank == iota(1).astype(f32))
    found = jnp.sum(sel.astype(f32), axis=0, keepdims=True)
    index = jnp.sum(jnp.where(sel, iota(0).astype(f32), 0.0), axis=0, keepdims=True)
    return jnp.where(found > 0.5, index, fill).astype(i32)


def ranked(rows, base, rank):
    out = []
    for q in range(4):
        sel = jnp.broadcast_to(rows[q : q + 1, :] - base, (BLK, BLK)) == iota(0)
        out.append(jnp.sum(jnp.where(sel, rank, 0.0), axis=0, keepdims=True))
    return jnp.concatenate(out, axis=0).astype(i32)


def gather_ids(n, me, refs, sems):
    loads = []
    for i, (ids, ids_v) in enumerate(refs):
        for r in range(5):
            e = jnp.clip(me + (r - 2), 0, n - 1)
            loads.append(pltpu.make_async_copy(ids.at[e], ids_v.at[r], sems.at[5 * i + r]))
    for c in loads:
        c.start()
    for c in loads:
        c.wait()


def pack_flows(src_v, list_s, outs, sems):
    for f, out in enumerate(outs):

        def send(r, carry, f=f, out=out):
            for u in range(8):
                b = list_s[f, r * 8 + u]
                pltpu.make_async_copy(src_v.at[b], out.at[r * 8 + u], sems.at[f]).start()
            return carry

        lax.fori_loop(0, CS // 8, send, 0)


def await_flows(src_v, outs, sems):
    for f, out in enumerate(outs):
        pltpu.make_async_copy(src_v.at[pl.ds(0, CS)], out, sems.at[f]).wait()


def far_kernel(n, sids, src, px, sid_v, src_v, list_v, list_s, sems, fsem):
    me = lax.axis_index(AXES)
    fetch = pltpu.make_async_copy(src, src_v, sems.at[10])
    fetch.start()
    gather_ids(n, me, ((sids, sid_v),), sems)
    side = 1 - 2 * (me % 2)
    present = presence(sid_v[2 + 2 * side], me * SB, SB)
    list_v[0:1, :] = listed(present, ranks(present), 0.0)
    move = pltpu.make_async_copy(list_v, list_s, sems.at[11])
    move.start()
    move.wait()
    fetch.wait()
    pack_flows(src_v, list_s, (px,), fsem)
    await_flows(src_v, (px,), fsem)


def near_kernel(n, sids, tids, src, py, pn, pd, plan, recv, sid_v, tid_v, src_v, list_v, list_s, sems, fsem):
    me = lax.axis_index(AXES)
    side = 1 - 2 * (me % 2)
    fetch = pltpu.make_async_copy(src, src_v, sems.at[10])
    fetch.start()
    gather_ids(n, me, ((sids, sid_v), (tids, tid_v)), sems)
    for f, rel in enumerate((-2 * side, -side, side)):
        present = presence(sid_v[2 + rel], me * SB, SB)
        list_v[f : f + 1, :] = listed(present, ranks(present), 0.0)
    move = pltpu.make_async_copy(list_v, list_s, sems.at[11])
    move.start()
    move.wait()
    fetch.wait()
    pack_flows(src_v, list_s, (py, pn, pd), fsem)

    own = sid_v[2]
    rel_of = own // SB - me
    pos = own - me * SB
    order = (0, -2 * side, 2 * side, side, -side)
    group = jnp.zeros((4, BLK), i32)
    for f, rel in enumerate(order[1:]):
        base = (me + rel) * SB
        rank = ranked(own, base, ranks(presence(own, base, SB)))
        here = rel_of == rel
        pos = jnp.where(here, rank, pos)
        group = jnp.where(here, f + 1, group)
    town = tid_v[2]
    trel = town // TB - me
    slot = jnp.zeros((4, BLK), i32)
    for f, rel in enumerate((0, 2 * side, -2 * side, side, -side)):
        base = (me + rel) * TB
        rank = ranked(town, base, ranks(presence(town, base, TB)))
        slot = jnp.where(trel == rel, rank + f * CT, slot)
    k = lax.broadcasted_iota(i32, (4, BLK), 0) * BLK + lax.broadcasted_iota(i32, (4, BLK), 1)
    entry = k + pos * 512 + slot * (1 << 16)

    upper = (iota(0) <= iota(1)).astype(bf16)
    dest = jnp.zeros((4, BLK), f32)
    start = jnp.zeros((1, 1), f32)
    heads = jnp.zeros((1, BLK), f32)
    lane = lax.broadcasted_iota(i32, (1, BLK), 1)
    for c in range(5):
        here = (group == c).astype(f32)
        run = jnp.dot(here.astype(bf16), upper, preferred_element_type=f32)
        rows = []
        total = jnp.zeros((1, 1), f32)
        for q in range(4):
            rows.append(run[q : q + 1, :] + total)
            total = total + run[q : q + 1, BLK - 1 : BLK]
        dest = jnp.where(here > 0.5, start + jnp.concatenate(rows, axis=0) - 1.0, dest)
        groups = jnp.floor((total + (GROUP - 1)) * (1.0 / GROUP))
        heads = jnp.where(lane == c, start, heads)
        heads = jnp.where(lane == 8 + c, groups, heads)
        start = start + groups * GROUP
    cols_d = jnp.transpose(jnp.concatenate([dest, entry.astype(f32)], axis=0))
    for p in range(5):
        at = (iota(1) + p * BLK).astype(f32)
        best = jnp.zeros((1, BLK), f32)
        seen = jnp.zeros((1, BLK), f32)
        for q in range(4):
            hit = jnp.broadcast_to(cols_d[:, q : q + 1], (BLK, BLK)) == at
            val = jnp.broadcast_to(cols_d[:, 4 + q : 5 + q], (BLK, BLK))
            best = best + jnp.sum(jnp.where(hit, val, 0.0), axis=0, keepdims=True)
            seen = seen + jnp.sum(hit.astype(f32), axis=0, keepdims=True)
        plan[p : p + 1, :] = jnp.where(seen > 0.5, best, float(TRASH << 16)).astype(i32)
    plan[5:6, :] = heads.astype(i32)

    for f, rel in enumerate(order):
        present = presence(tid_v[2 + rel], me * TB, TB)
        e = me + rel
        present = jnp.where((e >= 0) & (e < n), present, 0.0)
        recv[f : f + 1, :] = listed(present, ranks(present), float(TB))
    await_flows(src_v, (py, pn, pd), fsem)


any_spec = pl.BlockSpec(memory_space=pl.ANY)
sm_spec = pl.BlockSpec(memory_space=pltpu.SMEM)
vm_spec = pl.BlockSpec(memory_space=pltpu.VMEM)
flow_shape = jax.ShapeDtypeStruct((CS, BLK, BLK), bf16)


def cost(flops):
    return pl.CostEstimate(flops=flops, bytes_accessed=8_000_000, transcendentals=0)


def index_scratch(tables):
    return [pltpu.VMEM((5, 4, BLK), i32)] * tables + [
        pltpu.VMEM((SB, BLK, BLK), bf16),
        pltpu.VMEM((8, BLK), i32),
        pltpu.SMEM((8, BLK), i32),
        pltpu.SemaphoreType.DMA((12,)),
        pltpu.SemaphoreType.DMA((3,)),
    ]


def call_far(n, sids, src):
    return pl.pallas_call(
        functools.partial(far_kernel, n),
        out_shape=flow_shape,
        in_specs=[any_spec] * 2,
        out_specs=any_spec,
        scratch_shapes=index_scratch(1),
        name="far",
        cost_estimate=cost(1_000_000),
    )(sids, src)


def call_near(n, sids, tids, src):
    table = jax.ShapeDtypeStruct((8, BLK), i32)
    return pl.pallas_call(
        functools.partial(near_kernel, n),
        out_shape=[flow_shape] * 3 + [table] * 2,
        in_specs=[any_spec] * 3,
        out_specs=[any_spec] * 3 + [vm_spec] * 2,
        scratch_shapes=index_scratch(2),
        name="near",
        cost_estimate=cost(500_000_000),
    )(sids, tids, src)


def products(plan, cls, w, tab, acc):
    first = plan[5, cls]

    def step(g, carry):
        parts = []
        slots = []
        for u in range(GROUP):
            at = first + g * GROUP + u
            entry = plan[at >> 7, at & 127]
            slots.append(entry >> 16)
            parts.append(jnp.dot(w[entry & 511], tab[(entry >> 9) & 127], preferred_element_type=f32))
        for u in range(GROUP):
            acc[slots[u]] = acc[slots[u]] + parts[u]
        return carry

    lax.fori_loop(0, plan[5, 8 + cls], step, 0)


def first_kernel(plan, w, src, acc):
    def clear(i, carry):
        acc[i] = jnp.zeros((BLK, BLK), f32)
        return carry

    lax.fori_loop(0, SLOTS, clear, 0)
    products(plan, 0, w, src, acc)


acc_shape = jax.ShapeDtypeStruct((SLOTS, BLK, BLK), f32)


def call_first(plan, w, src):
    return pl.pallas_call(
        first_kernel,
        out_shape=acc_shape,
        in_specs=[sm_spec, vm_spec, vm_spec],
        out_specs=vm_spec,
        name="own",
        compiler_params=pltpu.CompilerParams(vmem_limit_bytes=VLIM),
        cost_estimate=cost(2_000_000_000),
    )(plan, w, src)


def second_kernel(plan, w, a, b, c, acc_in, acc):
    for i, tab in enumerate((a, b, c)):
        products(plan, 1 + i, w, tab, acc)


def call_second(plan, w, a, b, c, acc):
    return pl.pallas_call(
        second_kernel,
        out_shape=acc_shape,
        in_specs=[sm_spec] + [vm_spec] * 5,
        out_specs=vm_spec,
        input_output_aliases={5: 0},
        name="mid",
        compiler_params=pltpu.CompilerParams(vmem_limit_bytes=VLIM),
        cost_estimate=cost(2_000_000_000),
    )(plan, w, a, b, c, acc)


def third_kernel(plan, w, a, acc_in, acc):
    products(plan, 4, w, a, acc)


def call_third(plan, w, a, acc):
    return pl.pallas_call(
        third_kernel,
        out_shape=acc_shape,
        in_specs=[sm_spec] + [vm_spec] * 3,
        out_specs=vm_spec,
        input_output_aliases={3: 0},
        name="last",
        compiler_params=pltpu.CompilerParams(vmem_limit_bytes=VLIM),
        cost_estimate=cost(1_000_000_000),
    )(plan, w, a, acc)


def exchange_kernel(n, ny, acc, got, qbuf, send_sem, recv_sem):
    me = lax.axis_index(AXES)
    side = 1 - 2 * (me % 2)
    barrier = pltpu.get_barrier_semaphore()
    peers = [me + 2 * side, me - 2 * side, me - side, me + side]
    valid = [(p >= 0) & (p < n) for p in peers]
    count = 0
    for p, ok in zip(peers, valid):
        count = count + ok.astype(i32)

        @pl.when(ok)
        def _(p=p):
            pl.semaphore_signal(barrier, inc=1, device_id=(p // ny, p % ny), device_id_type=pl.DeviceIdType.MESH)

    half = CT // 2
    slots = (1, 2, 4, 3)
    comes = [valid[1], valid[0], valid[2], valid[3]]

    def quantize(c):
        f, h = c // 2, c % 2

        def one(s, carry):
            x = acc[slots[f] * CT + h * half + s]
            top = jnp.max(jnp.abs(x), axis=0, keepdims=True)
            e = jnp.ceil(jnp.log2(jnp.maximum(top, 1e-30)))
            q = jnp.clip(jnp.round(x * jnp.exp2(15.0 - e)), -32767.0, 32767.0)
            row = pl.multiple_of(s * BLK, BLK)
            qbuf[c, pl.ds(row, BLK), :] = q.astype(i32).astype(jnp.int16)
            return jnp.where(lax.broadcasted_iota(i32, (16, BLK), 0) == s, e.astype(i32), carry)

        exps = lax.fori_loop(0, half, one, jnp.zeros((16, BLK), i32))
        qbuf[c, pl.ds(half * BLK, 16), :] = exps.astype(jnp.int16)

    def copy(c):
        p = peers[c // 2]
        return pltpu.make_async_remote_copy(
            src_ref=qbuf.at[c],
            dst_ref=got.at[c],
            send_sem=send_sem.at[c],
            recv_sem=recv_sem.at[c],
            device_id=(p // ny, p % ny),
            device_id_type=pl.DeviceIdType.MESH,
        )

    def send(c):
        @pl.when(valid[c // 2])
        def _():
            copy(c).start()

    quantize(0)
    pl.semaphore_wait(barrier, count)
    for c in range(1, 8):
        quantize(c)
        send(c - 1)
    send(7)
    for c in range(8):

        @pl.when(valid[c // 2])
        def _(c=c):
            copy(c).wait_send()

        @pl.when(comes[c // 2])
        def _(c=c):
            copy(c).wait_recv()


def call_exchange(n, ny, acc):
    shape = (8, HALF_ROWS, BLK)
    return pl.pallas_call(
        functools.partial(exchange_kernel, n, ny),
        out_shape=jax.ShapeDtypeStruct(shape, jnp.int16),
        in_specs=[vm_spec],
        out_specs=vm_spec,
        scratch_shapes=[
            pltpu.VMEM(shape, jnp.int16),
            pltpu.SemaphoreType.DMA((8,)),
            pltpu.SemaphoreType.DMA((8,)),
        ],
        name="exchange",
        compiler_params=pltpu.CompilerParams(vmem_limit_bytes=VLIM, collective_id=0, has_side_effects=True),
        cost_estimate=cost(1_000_000_000),
    )(acc)


def final_kernel(recv, own, got, out, total, stage, sems):
    def clear(i, carry):
        total[i] = jnp.zeros((BLK, BLK), f32)
        return carry

    lax.fori_loop(0, TB, clear, 0)

    def add_own(r, carry):
        total[recv[0, r]] = own[r]
        return carry

    lax.fori_loop(0, CT, add_own, 0)
    half = CT // 2
    for c in range(8):
        scale = jnp.exp2(got[c, pl.ds(half * BLK, 16), :].astype(f32) - 15.0)
        for r in range(half):
            t = recv[(1, 2, 4, 3)[c // 2], (c % 2) * half + r]
            total[t] = total[t] + got[c, pl.ds(r * BLK, BLK), :].astype(f32) * scale[r : r + 1, :]
    step = TB // 4
    writes = []
    for j in range(4):

        def store(i, carry):
            stage[i] = total[i].astype(bf16)
            return carry

        lax.fori_loop(j * step, (j + 1) * step, store, 0)
        at = pl.ds(j * step, step)
        writes.append(pltpu.make_async_copy(stage.at[at], out.at[at], sems.at[j]))
        if j:
            writes[j - 1].start()
    writes[3].start()
    for x in writes:
        x.wait()


def call_final(recv, own, got):
    return pl.pallas_call(
        final_kernel,
        out_shape=jax.ShapeDtypeStruct((TB, BLK, BLK), bf16),
        in_specs=[sm_spec, vm_spec, vm_spec],
        out_specs=any_spec,
        scratch_shapes=[
            pltpu.VMEM((TB + 1, BLK, BLK), f32),
            pltpu.VMEM((TB, BLK, BLK), bf16),
            pltpu.SemaphoreType.DMA((4,)),
        ],
        name="final",
        compiler_params=pltpu.CompilerParams(vmem_limit_bytes=VLIM),
        cost_estimate=cost(100_000_000),
    )(recv, own, got)


def swaps(n):
    def pairs(step):
        moves = [(d, d + step * (1 - 2 * (d % 2))) for d in range(n)]
        return [(d, t) for d, t in moves if 0 <= t < n]

    return pairs(2), pairs(-2), pairs(-1), pairs(1)


def body(source_field, weight_blocks, source_ids, target_ids):
    n = lax.axis_size(AXES)
    out_two, in_two, across, partner = swaps(n)
    sids = source_ids.reshape(n, 4, BLK)
    tids = target_ids.reshape(n, 4, BLK)
    send = lambda x, pairs: lax.ppermute(x, AXES, pairs)
    a = send(call_far(n, sids, source_field), out_two)
    py, pn, pd, plan, recv = call_near(n, sids, tids, source_field)
    b = send(py, in_two)
    d = send(pn, across)
    c = send(pd, partner)
    acc = call_first(plan, weight_blocks, source_field)
    acc = call_second(plan, weight_blocks, a, b, c, acc)
    acc = call_third(plan, weight_blocks, d, acc)
    got = call_exchange(n, lax.axis_size("gy"), acc)
    return call_final(recv, acc, got)


def solution(mesh):
    return jax.shard_map(
        body,
        mesh=mesh,
        in_specs=(P(AXES, None, None), P(AXES, None, None), P(), P()),
        out_specs=P(AXES, None, None),
        check_vma=False,
    )
```

```python
import functools

import jax
import jax.numpy as jnp
from jax import lax
from jax.experimental import pallas as pl
from jax.experimental.pallas import tpu as pltpu
from jax.sharding import PartitionSpec as P


BLK = 128
SB = 128
TB = 64
WB = 512
CS = 64
CT = 16
AXES = ("gx", "gy")
TRASH = 80
SLOTS = 84
GROUP = 16
PART = 54
PART_B = 52
UNION = PART + PART_B
TAIL = SB - UNION
FAR = 44
REST = CS - FAR
HEADS = 6
VLIM = 9
CHUNKS = 8
HALF_ROWS = CT // 2 * BLK + 16


f32 = jnp.float32
i32 = jnp.int32
bf16 = jnp.bfloat16


def iota(dim):
    return lax.broadcasted_iota(i32, (BLK, BLK), dim)


def presence(rows, base, limit):
    sub = iota(0)
    hits = jnp.zeros((BLK, BLK), f32)
    for q in range(4):
        hits = hits + (jnp.broadcast_to(rows[q : q + 1, :] - base, (BLK, BLK)) == sub).astype(f32)
    count = jnp.dot(hits.astype(bf16), jnp.ones((BLK, BLK), bf16), preferred_element_type=f32)
    return ((count > 0.5) & (sub < limit)).astype(f32)


def ranks(present):
    lower = (iota(1) < iota(0)).astype(bf16)
    return jnp.dot(lower, present.astype(bf16), preferred_element_type=f32)


def listed(present, rank, fill):
    sel = (present > 0.5) & (rank == iota(1).astype(f32))
    found = jnp.sum(sel.astype(f32), axis=0, keepdims=True)
    index = jnp.sum(jnp.where(sel, iota(0).astype(f32), 0.0), axis=0, keepdims=True)
    return jnp.where(found > 0.5, index, fill).astype(i32)


def ranked(rows, base, rank):
    out = []
    for q in range(4):
        sel = jnp.broadcast_to(rows[q : q + 1, :] - base, (BLK, BLK)) == iota(0)
        out.append(jnp.sum(jnp.where(sel, rank, 0.0), axis=0, keepdims=True))
    return jnp.concatenate(out, axis=0).astype(i32)


def gather_ids(n, me, refs, sems):
    loads = []
    for i, (ids, ids_v) in enumerate(refs):
        for r in range(5):
            e = jnp.clip(me + (r - 2), 0, n - 1)
            loads.append(pltpu.make_async_copy(ids.at[e], ids_v.at[r], sems.at[5 * i + r]))
    for c in loads:
        c.start()
    for c in loads:
        c.wait()


def pack(src_v, list_s, row, first, out, count):
    def move(r, carry):
        for u in range(2):
            out[r * 2 + u] = src_v[list_s[row, first + r * 2 + u]]
        return carry

    lax.fori_loop(0, count // 2, move, 0)


def either(one, other, base):
    return jnp.maximum(presence(one, base, SB), presence(other, base, SB))


def union_kernel(n, sids, src, pn, sid_v, src_v, list_v, list_s, sems):
    me = lax.axis_index(AXES)
    side = 1 - 2 * (me % 2)
    loads = []
    for r in (2 - side, 2 - 2 * side):
        e = jnp.clip(me + (r - 2), 0, n - 1)
        loads.append(pltpu.make_async_copy(sids.at[e], sid_v.at[r], sems.at[len(loads)]))
        loads[-1].start()
    fetch = pltpu.make_async_copy(src, src_v, sems.at[10])
    fetch.start()
    for x in loads:
        x.wait()
    base = me * SB
    present = either(sid_v[2 - side], sid_v[2 - 2 * side], base)
    list_v[...] = listed(present, ranks(present), 0.0)
    move = pltpu.make_async_copy(list_v, list_s, sems.at[11])
    move.start()
    move.wait()
    fetch.wait()

    def send(r, carry):
        for u in range(6):
            b = list_s[0, r * 6 + u]
            pltpu.make_async_copy(src_v.at[b], pn.at[r * 6 + u], sems.at[2]).start()
        return carry

    lax.fori_loop(0, PART // 6, send, 0)
    pltpu.make_async_copy(src_v.at[pl.ds(0, PART)], pn, sems.at[2]).wait()


def plan_kernel(n, sids, tids, src_v, py, px, pz, pd, pt, plan, recv, sid_v, tid_v, list_v, list_s, sems):
    me = lax.axis_index(AXES)
    side = 1 - 2 * (me % 2)
    gather_ids(n, me, ((sids, sid_v), (tids, tid_v)), sems)
    base = me * SB
    for f, rel in enumerate((2 * side, side)):
        present = presence(sid_v[2 + rel], base, SB)
        list_v[f : f + 1, :] = listed(present, ranks(present), 0.0)
    present = either(sid_v[2 - side], sid_v[2 - 2 * side], base)
    list_v[2:3, :] = listed(present, ranks(present), 0.0)
    move = pltpu.make_async_copy(list_v, list_s, sems.at[11])
    move.start()

    own = sid_v[2]
    rel_of = own // SB - me
    pos = own - me * SB
    group = jnp.zeros((4, BLK), i32)
    for c, rel in ((6, -2 * side), (3, side)):
        base = (me + rel) * SB
        rank = ranked(own, base, ranks(presence(own, base, SB)))
        here = rel_of == rel
        late = (rank >= FAR) & (c == 6)
        pos = jnp.where(here, jnp.where(late, rank - FAR, rank), pos)
        group = jnp.where(here, jnp.where(late, 9, c), group)
    for lo, hi, over, rel in ((1, 5, 7, -side), (2, 4, 8, 2 * side)):
        base = (me + rel) * SB
        rank = ranked(own, base, ranks(either(own, sid_v[2 + side], base)))
        here = rel_of == rel
        part = (rank >= PART).astype(i32) + (rank >= UNION).astype(i32)
        pos = jnp.where(here, rank - jnp.where(part == 0, 0, jnp.where(part == 1, PART, UNION)), pos)
        group = jnp.where(here, jnp.where(part == 0, lo, jnp.where(part == 1, hi, over)), group)
    town = tid_v[2]
    trel = town // TB - me
    slot = jnp.zeros((4, BLK), i32)
    for f, rel in enumerate((0, 2 * side, -2 * side, side, -side)):
        base = (me + rel) * TB
        rank = ranked(town, base, ranks(presence(town, base, TB)))
        slot = jnp.where(trel == rel, rank + f * CT, slot)
    k = lax.broadcasted_iota(i32, (4, BLK), 0) * BLK + lax.broadcasted_iota(i32, (4, BLK), 1)
    entry = k + pos * 512 + slot * (1 << 16)

    upper = (iota(0) <= iota(1)).astype(bf16)
    dest = jnp.zeros((4, BLK), f32)
    start = jnp.zeros((1, 1), f32)
    heads = jnp.zeros((1, BLK), f32)
    lane = lax.broadcasted_iota(i32, (1, BLK), 1)
    for c in range(10):
        here = (group == c).astype(f32)
        run = jnp.dot(here.astype(bf16), upper, preferred_element_type=f32)
        rows = []
        total = jnp.zeros((1, 1), f32)
        for q in range(4):
            rows.append(run[q : q + 1, :] + total)
            total = total + run[q : q + 1, BLK - 1 : BLK]
        dest = jnp.where(here > 0.5, start + jnp.concatenate(rows, axis=0) - 1.0, dest)
        groups = jnp.floor((total + (GROUP - 1)) * (1.0 / GROUP))
        heads = jnp.where(lane == c, start, heads)
        heads = jnp.where(lane == 16 + c, groups, heads)
        start = start + groups * GROUP
    cols_d = jnp.transpose(jnp.concatenate([dest, entry.astype(f32)], axis=0))
    for p in range(HEADS):
        at = (iota(1) + p * BLK).astype(f32)
        best = jnp.zeros((1, BLK), f32)
        seen = jnp.zeros((1, BLK), f32)
        for q in range(4):
            hit = jnp.broadcast_to(cols_d[:, q : q + 1], (BLK, BLK)) == at
            val = jnp.broadcast_to(cols_d[:, 4 + q : 5 + q], (BLK, BLK))
            best = best + jnp.sum(jnp.where(hit, val, 0.0), axis=0, keepdims=True)
            seen = seen + jnp.sum(hit.astype(f32), axis=0, keepdims=True)
        plan[p : p + 1, :] = jnp.where(seen > 0.5, best, float(TRASH << 16)).astype(i32)
    plan[HEADS : HEADS + 1, :] = heads.astype(i32)

    for f, rel in enumerate((0, -2 * side, 2 * side, side, -side)):
        present = presence(tid_v[2 + rel], me * TB, TB)
        e = me + rel
        present = jnp.where((e >= 0) & (e < n), present, 0.0)
        recv[f : f + 1, :] = listed(present, ranks(present), float(TB))

    move.wait()
    pack(src_v, list_s, 2, PART, py, PART_B)
    pack(src_v, list_s, 0, 0, px, FAR)
    pack(src_v, list_s, 0, FAR, pz, REST)
    pack(src_v, list_s, 1, 0, pd, CS)
    pack(src_v, list_s, 2, UNION, pt, TAIL)


def excess_kernel(ids, flag):
    sub = lax.broadcasted_iota(i32, (8, BLK), 0)
    lane = lax.broadcasted_iota(i32, (8, BLK), 1)
    even = lane % 2 == 0
    owners = [lane - lane % 2 - 1, lane - lane % 2 + 2]
    bits = [[jnp.zeros((8, BLK), i32) for _ in range(4)] for _ in range(2)]
    for q in range(4):
        turned = jnp.transpose(ids[:, q, :].astype(f32)).astype(i32)
        for r in range(BLK // 8):
            rows = turned[r * 8 : r * 8 + 8, :]
            for o in range(2):
                local = rows - owners[o] * SB
                word = local >> 5
                bit = jnp.left_shift(jnp.ones_like(local), local & 31)
                for v in range(4):
                    bits[o][v] = bits[o][v] | jnp.where(word == v, bit, 0)
    worst = sub * 0
    for o in range(2):
        total = sub * 0
        for v in range(4):
            x = bits[o][v]
            for step in (4, 2, 1):
                x = x | pltpu.roll(x, step, 0)
            x = x | jnp.where(even, pltpu.roll(x, BLK - 1, 1), pltpu.roll(x, 1, 1))
            total = total + lax.population_count(x)
        worst = jnp.maximum(worst, total)
    worst = jnp.max(worst.astype(f32), axis=1, keepdims=True)
    flag[...] = jnp.broadcast_to((worst > UNION).astype(i32), (8, BLK))


any_spec = pl.BlockSpec(memory_space=pltpu.HBM)
sm_spec = pl.BlockSpec(memory_space=pltpu.SMEM)
vm_spec = pl.BlockSpec(memory_space=pltpu.VMEM)


def blocks(count):
    return jax.ShapeDtypeStruct((count, BLK, BLK), bf16)


def cost(flops):
    return pl.CostEstimate(flops=flops, bytes_accessed=8_000_000, transcendentals=0)


def index_scratch(*more):
    return [
        *more,
        pltpu.VMEM((8, BLK), i32),
        pltpu.SMEM((8, BLK), i32),
        pltpu.SemaphoreType.DMA((12,)),
    ]


def limit(mib):
    return pltpu.CompilerParams(vmem_limit_bytes=mib * 1024 * 1024)


def call_union(n, sids, src):
    return pl.pallas_call(
        functools.partial(union_kernel, n),
        out_shape=blocks(PART),
        in_specs=[any_spec] * 2,
        out_specs=any_spec,
        scratch_shapes=[
            pltpu.VMEM((5, 4, BLK), i32),
            pltpu.VMEM((SB, BLK, BLK), bf16),
            pltpu.VMEM((1, BLK), i32),
            pltpu.SMEM((1, BLK), i32),
            pltpu.SemaphoreType.DMA((12,)),
        ],
        name="union",
        cost_estimate=cost(1_000_000),
    )(sids, src)


def call_plan(n, sids, tids, src):
    table = jax.ShapeDtypeStruct((8, BLK), i32)
    return pl.pallas_call(
        functools.partial(plan_kernel, n),
        out_shape=[blocks(c) for c in (PART_B, FAR, REST, CS, TAIL)] + [table] * 2,
        in_specs=[any_spec, any_spec, vm_spec],
        out_specs=[vm_spec] * 7,
        scratch_shapes=index_scratch(*[pltpu.VMEM((5, 4, BLK), i32)] * 2),
        name="plan",
        compiler_params=limit(16),
        cost_estimate=cost(500_000_000),
    )(sids, tids, src)


def call_excess(ids):
    return pl.pallas_call(
        excess_kernel,
        out_shape=jax.ShapeDtypeStruct((8, BLK), i32),
        in_specs=[vm_spec],
        out_specs=vm_spec,
        name="excess",
        compiler_params=limit(4),
        cost_estimate=cost(500_000_000),
    )(ids)


def products(plan, cls, w, tab, acc):
    first = plan[HEADS, cls]

    def step(g, carry):
        parts = []
        slots = []
        for u in range(GROUP):
            at = first + g * GROUP + u
            entry = plan[at >> 7, at & 127]
            slots.append(entry >> 16)
            parts.append(jnp.dot(w[entry & 511], tab[(entry >> 9) & 127], preferred_element_type=f32))
        for u in range(GROUP):
            acc[slots[u]] = acc[slots[u]] + parts[u]
        return carry

    lax.fori_loop(0, plan[HEADS, 16 + cls], step, 0)


def first_kernel(plan, w_hbm, src, acc, w, sems):
    step = WB // CHUNKS
    loads = []
    for i in range(CHUNKS):
        at = pl.ds(i * step, step)
        loads.append(pltpu.make_async_copy(w_hbm.at[at], w.at[at], sems.at[i]))
        loads[i].start()

    def clear(i, carry):
        acc[i] = jnp.zeros((BLK, BLK), f32)
        return carry

    lax.fori_loop(0, SLOTS, clear, 0)
    for x in loads:
        x.wait()
    products(plan, 0, w, src, acc)


acc_shape = jax.ShapeDtypeStruct((SLOTS, BLK, BLK), f32)


def call_first(plan, w, src):
    return pl.pallas_call(
        first_kernel,
        out_shape=[acc_shape, blocks(WB)],
        in_specs=[sm_spec, any_spec, vm_spec],
        out_specs=[vm_spec, vm_spec],
        scratch_shapes=[pltpu.SemaphoreType.DMA((CHUNKS,))],
        name="own",
        compiler_params=limit(24),
        cost_estimate=cost(2_000_000_000),
    )(plan, w, src)


def more_kernel(classes, plan, w, *refs):
    acc = refs[-1]
    for cls, tab in zip(classes, refs):
        products(plan, cls, w, tab, acc)


def call_more(classes, plan, w, tables, acc):
    return pl.pallas_call(
        functools.partial(more_kernel, classes),
        out_shape=acc_shape,
        in_specs=[sm_spec] + [vm_spec] * (2 + len(tables)),
        out_specs=vm_spec,
        input_output_aliases={2 + len(tables): 0},
        compiler_params=limit(VLIM),
        cost_estimate=cost(1_000_000_000),
    )(plan, w, *tables, acc)


def exchange_kernel(n, ny, acc, got, qbuf, send_sem, recv_sem):
    me = lax.axis_index(AXES)
    side = 1 - 2 * (me % 2)
    barrier = pltpu.get_barrier_semaphore()
    peers = [me + 2 * side, me - 2 * side, me - side, me + side]
    valid = [(p >= 0) & (p < n) for p in peers]
    count = 0
    for p, ok in zip(peers, valid):
        count = count + ok.astype(i32)

        @pl.when(ok)
        def _(p=p):
            pl.semaphore_signal(barrier, inc=1, device_id=(p // ny, p % ny), device_id_type=pl.DeviceIdType.MESH)

    half = CT // 2
    slots = (1, 2, 4, 3)
    comes = [valid[1], valid[0], valid[2], valid[3]]

    def quantize(c):
        f, h = c // 2, c % 2

        def four(g, carry):
            for u in range(4):
                s = g * 4 + u
                x = acc[slots[f] * CT + h * half + s]
                top = jnp.max(jnp.abs(x), axis=0, keepdims=True)
                e = jnp.ceil(jnp.log2(jnp.maximum(top, 1e-30)))
                q = jnp.clip(jnp.round(x * jnp.exp2(15.0 - e)), -32767.0, 32767.0)
                row = pl.multiple_of(s * BLK, BLK)
                qbuf[c, pl.ds(row, BLK), :] = q.astype(i32).astype(jnp.int16)
                carry = jnp.where(lax.broadcasted_iota(i32, (16, BLK), 0) == s, e.astype(i32), carry)
            return carry

        exps = lax.fori_loop(0, half // 4, four, jnp.zeros((16, BLK), i32))
        qbuf[c, pl.ds(half * BLK, 16), :] = exps.astype(jnp.int16)

    def copy(c):
        p = peers[c // 2]
        return pltpu.make_async_remote_copy(
            src_ref=qbuf.at[c],
            dst_ref=got.at[c],
            send_sem=send_sem.at[c],
            recv_sem=recv_sem.at[c],
            device_id=(p // ny, p % ny),
            device_id_type=pl.DeviceIdType.MESH,
        )

    def send(c):
        @pl.when(valid[c // 2])
        def _():
            copy(c).start()

    quantize(0)
    quantize(1)
    pl.semaphore_wait(barrier, count)
    for c in range(1, 8):
        if c > 1:
            quantize(c)
        send(c - 1)
    send(7)

    for c in range(8):

        @pl.when(valid[c // 2])
        def _(c=c):
            copy(c).wait_send()

        @pl.when(comes[c // 2])
        def _(c=c):
            copy(c).wait_recv()


def call_exchange(n, ny, acc):
    shape = (8, HALF_ROWS, BLK)
    return pl.pallas_call(
        functools.partial(exchange_kernel, n, ny),
        out_shape=jax.ShapeDtypeStruct(shape, jnp.int16),
        in_specs=[vm_spec],
        out_specs=vm_spec,
        scratch_shapes=[
            pltpu.VMEM(shape, jnp.int16),
            pltpu.SemaphoreType.DMA((8,)),
            pltpu.SemaphoreType.DMA((8,)),
        ],
        name="exchange",
        compiler_params=pltpu.CompilerParams(vmem_limit_bytes=VLIM * 1024 * 1024, collective_id=0, has_side_effects=True),
        cost_estimate=cost(1_000_000_000),
    )(acc)


def final_kernel(recv, own, got, out, total, stage, sems):
    def clear(i, carry):
        total[i] = jnp.zeros((BLK, BLK), f32)
        return carry

    lax.fori_loop(0, TB, clear, 0)

    def add_own(r, carry):
        total[recv[0, r]] = own[r]
        return carry

    lax.fori_loop(0, CT, add_own, 0)
    half = CT // 2
    for c in range(8):
        scale = jnp.exp2(got[c, pl.ds(half * BLK, 16), :].astype(f32) - 15.0)
        for r in range(half):
            t = recv[(1, 2, 4, 3)[c // 2], (c % 2) * half + r]
            total[t] = total[t] + got[c, pl.ds(r * BLK, BLK), :].astype(f32) * scale[r : r + 1, :]
    step = TB // 4
    writes = []
    for j in range(4):

        def store(i, carry):
            stage[i] = total[i].astype(bf16)
            return carry

        lax.fori_loop(j * step, (j + 1) * step, store, 0)
        at = pl.ds(j * step, step)
        writes.append(pltpu.make_async_copy(stage.at[at], out.at[at], sems.at[j]))
        if j:
            writes[j - 1].start()
    writes[3].start()
    for x in writes:
        x.wait()


def call_final(recv, own, got):
    return pl.pallas_call(
        final_kernel,
        out_shape=jax.ShapeDtypeStruct((TB, BLK, BLK), bf16),
        in_specs=[sm_spec, vm_spec, vm_spec],
        out_specs=any_spec,
        scratch_shapes=[
            pltpu.VMEM((TB + 1, BLK, BLK), f32),
            pltpu.VMEM((TB, BLK, BLK), bf16),
            pltpu.SemaphoreType.DMA((4,)),
        ],
        name="final",
        compiler_params=limit(VLIM),
        cost_estimate=cost(100_000_000),
    )(recv, own, got)


def swaps(n):
    def pairs(step):
        moves = [(d, d + step * (1 - 2 * (d % 2))) for d in range(n)]
        return [(d, t) for d, t in moves if 0 <= t < n]

    return pairs(2), pairs(-2), pairs(-1), pairs(1)


def remap(source_field, weight_blocks, source_ids, target_ids):
    n = lax.axis_size(AXES)
    out_two, in_two, across, partner = swaps(n)
    sids = source_ids.reshape(n, 4, BLK)
    tids = target_ids.reshape(n, 4, BLK)
    send = lambda x, pairs: lax.ppermute(x, AXES, pairs)
    pn = call_union(n, sids, source_field)
    got_n = send(pn, across)
    py, px, pz, pd, pt, plan, recv = call_plan(n, sids, tids, source_field)
    got_y = send(py, in_two)
    got_d = send(pd, partner)
    over = call_excess(sids)[0, 0] > 0
    tail_n, tail_y = lax.cond(
        over,
        lambda t: (send(t, across), send(t, in_two)),
        lambda t: (jnp.zeros_like(t), jnp.zeros_like(t)),
        pt,
    )
    plan, tail_n, tail_y = lax.optimization_barrier((plan, tail_n, tail_y))
    acc, w = call_first(plan, weight_blocks, source_field)
    px, pz, acc = lax.optimization_barrier((px, pz, acc))
    got_x = send(px, out_two)
    got_z = send(pz, out_two)
    swap_n = send(got_n, partner)
    acc = call_more((3, 1, 2), plan, w, (got_d, got_n, swap_n), acc)
    acc, got_y = lax.optimization_barrier((acc, got_y))
    swap_y = send(got_y, partner)
    acc = call_more((4, 5, 7, 8), plan, w, (got_y, swap_y, tail_n, tail_y), acc)
    acc = call_more((6,), plan, w, (got_x,), acc)
    acc = call_more((9,), plan, w, (got_z,), acc)
    got = call_exchange(n, lax.axis_size("gy"), acc)
    return call_final(recv, acc, got)


def solution(mesh):
    return jax.shard_map(
        remap,
        mesh=mesh,
        in_specs=(P(AXES, None, None), P(AXES, None, None), P(), P()),
        out_specs=P(AXES, None, None),
        check_vma=False,
    )
```

```python
import functools

import jax
import jax.numpy as jnp
from jax import lax
from jax.experimental import pallas as pl
from jax.experimental.pallas import tpu as pltpu
from jax.sharding import PartitionSpec as P


BLK = 128
SB = 128
TB = 64
WB = 512
CS = 64
CT = 16
AXES = ("gx", "gy")
TRASH = 80
SLOTS = 84
GROUP = 16
PART = 52
UNION = 2 * PART
TAIL = SB - UNION
FAR = 52
REST = CS - FAR
HEADS = 6
VLIM = 9
CHUNKS = 8
HALF_ROWS = CT // 2 * BLK + 16


f32 = jnp.float32
i32 = jnp.int32
bf16 = jnp.bfloat16


def iota(dim):
    return lax.broadcasted_iota(i32, (BLK, BLK), dim)


def presence(rows, base, limit):
    sub = iota(0)
    hits = jnp.zeros((BLK, BLK), f32)
    for q in range(4):
        hits = hits + (jnp.broadcast_to(rows[q : q + 1, :] - base, (BLK, BLK)) == sub).astype(f32)
    count = jnp.dot(hits.astype(bf16), jnp.ones((BLK, BLK), bf16), preferred_element_type=f32)
    return ((count > 0.5) & (sub < limit)).astype(f32)


def ranks(present):
    lower = (iota(1) < iota(0)).astype(bf16)
    return jnp.dot(lower, present.astype(bf16), preferred_element_type=f32)


def listed(present, rank, fill):
    sel = (present > 0.5) & (rank == iota(1).astype(f32))
    found = jnp.sum(sel.astype(f32), axis=0, keepdims=True)
    index = jnp.sum(jnp.where(sel, iota(0).astype(f32), 0.0), axis=0, keepdims=True)
    return jnp.where(found > 0.5, index, fill).astype(i32)


def ranked(rows, base, rank):
    out = []
    for q in range(4):
        sel = jnp.broadcast_to(rows[q : q + 1, :] - base, (BLK, BLK)) == iota(0)
        out.append(jnp.sum(jnp.where(sel, rank, 0.0), axis=0, keepdims=True))
    return jnp.concatenate(out, axis=0).astype(i32)


def gather_ids(n, me, refs, sems):
    loads = []
    for i, (ids, ids_v) in enumerate(refs):
        for r in range(5):
            e = jnp.clip(me + (r - 2), 0, n - 1)
            loads.append(pltpu.make_async_copy(ids.at[e], ids_v.at[r], sems.at[5 * i + r]))
    for c in loads:
        c.start()
    for c in loads:
        c.wait()


def pack(src_v, list_s, row, first, out, count):
    def move(r, carry):
        for u in range(2):
            out[r * 2 + u] = src_v[list_s[row, first + r * 2 + u]]
        return carry

    lax.fori_loop(0, count // 2, move, 0)


def either(one, other, base):
    return jnp.maximum(presence(one, base, SB), presence(other, base, SB))


def union_kernel(n, sids, src, pn, sid_v, src_v, list_v, list_s, sems):
    me = lax.axis_index(AXES)
    side = 1 - 2 * (me % 2)
    loads = []
    for r in (2 - side, 2 - 2 * side):
        e = jnp.clip(me + (r - 2), 0, n - 1)
        loads.append(pltpu.make_async_copy(sids.at[e], sid_v.at[r], sems.at[len(loads)]))
        loads[-1].start()
    fetch = pltpu.make_async_copy(src, src_v, sems.at[10])
    fetch.start()
    for x in loads:
        x.wait()
    base = me * SB
    present = either(sid_v[2 - side], sid_v[2 - 2 * side], base)
    list_v[...] = listed(present, ranks(present), 0.0)
    move = pltpu.make_async_copy(list_v, list_s, sems.at[11])
    move.start()
    move.wait()
    fetch.wait()

    def send(r, carry):
        for u in range(4):
            b = list_s[0, r * 4 + u]
            pltpu.make_async_copy(src_v.at[b], pn.at[r * 4 + u], sems.at[2]).start()
        return carry

    lax.fori_loop(0, PART // 4, send, 0)
    pltpu.make_async_copy(src_v.at[pl.ds(0, PART)], pn, sems.at[2]).wait()


def plan_kernel(n, sids, tids, src_v, py, px, pz, pd, pt, plan, recv, sid_v, tid_v, list_v, list_s, sems):
    me = lax.axis_index(AXES)
    side = 1 - 2 * (me % 2)
    gather_ids(n, me, ((sids, sid_v), (tids, tid_v)), sems)
    base = me * SB
    for f, rel in enumerate((2 * side, side)):
        present = presence(sid_v[2 + rel], base, SB)
        list_v[f : f + 1, :] = listed(present, ranks(present), 0.0)
    present = either(sid_v[2 - side], sid_v[2 - 2 * side], base)
    list_v[2:3, :] = listed(present, ranks(present), 0.0)
    move = pltpu.make_async_copy(list_v, list_s, sems.at[11])
    move.start()

    own = sid_v[2]
    rel_of = own // SB - me
    pos = own - me * SB
    group = jnp.zeros((4, BLK), i32)
    for c, rel in ((6, -2 * side), (3, side)):
        base = (me + rel) * SB
        rank = ranked(own, base, ranks(presence(own, base, SB)))
        here = rel_of == rel
        late = (rank >= FAR) & (c == 6)
        pos = jnp.where(here, jnp.where(late, rank - FAR, rank), pos)
        group = jnp.where(here, jnp.where(late, 9, c), group)
    for lo, hi, over, rel in ((1, 5, 7, -side), (2, 4, 8, 2 * side)):
        base = (me + rel) * SB
        rank = ranked(own, base, ranks(either(own, sid_v[2 + side], base)))
        here = rel_of == rel
        part = (rank >= PART).astype(i32) + (rank >= UNION).astype(i32)
        pos = jnp.where(here, rank - jnp.where(part == 0, 0, jnp.where(part == 1, PART, UNION)), pos)
        group = jnp.where(here, jnp.where(part == 0, lo, jnp.where(part == 1, hi, over)), group)
    town = tid_v[2]
    trel = town // TB - me
    slot = jnp.zeros((4, BLK), i32)
    for f, rel in enumerate((0, 2 * side, -2 * side, side, -side)):
        base = (me + rel) * TB
        rank = ranked(town, base, ranks(presence(town, base, TB)))
        slot = jnp.where(trel == rel, rank + f * CT, slot)
    k = lax.broadcasted_iota(i32, (4, BLK), 0) * BLK + lax.broadcasted_iota(i32, (4, BLK), 1)
    entry = k + pos * 512 + slot * (1 << 16)

    upper = (iota(0) <= iota(1)).astype(bf16)
    dest = jnp.zeros((4, BLK), f32)
    start = jnp.zeros((1, 1), f32)
    heads = jnp.zeros((1, BLK), f32)
    lane = lax.broadcasted_iota(i32, (1, BLK), 1)
    for c in range(10):
        here = (group == c).astype(f32)
        run = jnp.dot(here.astype(bf16), upper, preferred_element_type=f32)
        rows = []
        total = jnp.zeros((1, 1), f32)
        for q in range(4):
            rows.append(run[q : q + 1, :] + total)
            total = total + run[q : q + 1, BLK - 1 : BLK]
        dest = jnp.where(here > 0.5, start + jnp.concatenate(rows, axis=0) - 1.0, dest)
        groups = jnp.floor((total + (GROUP - 1)) * (1.0 / GROUP))
        heads = jnp.where(lane == c, start, heads)
        heads = jnp.where(lane == 16 + c, groups, heads)
        start = start + groups * GROUP
    cols_d = jnp.transpose(jnp.concatenate([dest, entry.astype(f32)], axis=0))
    for p in range(HEADS):
        at = (iota(1) + p * BLK).astype(f32)
        best = jnp.zeros((1, BLK), f32)
        seen = jnp.zeros((1, BLK), f32)
        for q in range(4):
            hit = jnp.broadcast_to(cols_d[:, q : q + 1], (BLK, BLK)) == at
            val = jnp.broadcast_to(cols_d[:, 4 + q : 5 + q], (BLK, BLK))
            best = best + jnp.sum(jnp.where(hit, val, 0.0), axis=0, keepdims=True)
            seen = seen + jnp.sum(hit.astype(f32), axis=0, keepdims=True)
        plan[p : p + 1, :] = jnp.where(seen > 0.5, best, float(TRASH << 16)).astype(i32)
    plan[HEADS : HEADS + 1, :] = heads.astype(i32)

    for f, rel in enumerate((0, -2 * side, 2 * side, side, -side)):
        present = presence(tid_v[2 + rel], me * TB, TB)
        e = me + rel
        present = jnp.where((e >= 0) & (e < n), present, 0.0)
        recv[f : f + 1, :] = listed(present, ranks(present), float(TB))

    move.wait()
    pack(src_v, list_s, 2, PART, py, PART)
    pack(src_v, list_s, 0, 0, px, FAR)
    pack(src_v, list_s, 0, FAR, pz, REST)
    pack(src_v, list_s, 1, 0, pd, CS)
    pack(src_v, list_s, 2, UNION, pt, TAIL)


def excess_kernel(ids, flag):
    sub = lax.broadcasted_iota(i32, (8, BLK), 0)
    lane = lax.broadcasted_iota(i32, (8, BLK), 1)
    even = lane % 2 == 0
    owners = [lane - lane % 2 - 1, lane - lane % 2 + 2]
    bits = [[jnp.zeros((8, BLK), i32) for _ in range(4)] for _ in range(2)]
    for q in range(4):
        turned = jnp.transpose(ids[:, q, :].astype(f32)).astype(i32)
        for r in range(BLK // 8):
            rows = turned[r * 8 : r * 8 + 8, :]
            for o in range(2):
                local = rows - owners[o] * SB
                word = local >> 5
                bit = jnp.left_shift(jnp.ones_like(local), local & 31)
                for v in range(4):
                    bits[o][v] = bits[o][v] | jnp.where(word == v, bit, 0)
    worst = sub * 0
    for o in range(2):
        total = sub * 0
        for v in range(4):
            x = bits[o][v]
            for step in (4, 2, 1):
                x = x | pltpu.roll(x, step, 0)
            x = x | jnp.where(even, pltpu.roll(x, BLK - 1, 1), pltpu.roll(x, 1, 1))
            total = total + lax.population_count(x)
        worst = jnp.maximum(worst, total)
    worst = jnp.max(worst.astype(f32), axis=1, keepdims=True)
    flag[...] = jnp.broadcast_to((worst > UNION).astype(i32), (8, BLK))


any_spec = pl.BlockSpec(memory_space=pltpu.HBM)
sm_spec = pl.BlockSpec(memory_space=pltpu.SMEM)
vm_spec = pl.BlockSpec(memory_space=pltpu.VMEM)


def blocks(count):
    return jax.ShapeDtypeStruct((count, BLK, BLK), bf16)


def cost(flops):
    return pl.CostEstimate(flops=flops, bytes_accessed=8_000_000, transcendentals=0)


def index_scratch(*more):
    return [
        *more,
        pltpu.VMEM((8, BLK), i32),
        pltpu.SMEM((8, BLK), i32),
        pltpu.SemaphoreType.DMA((12,)),
    ]


def limit(mib):
    return pltpu.CompilerParams(vmem_limit_bytes=mib * 1024 * 1024)


def call_union(n, sids, src):
    return pl.pallas_call(
        functools.partial(union_kernel, n),
        out_shape=blocks(PART),
        in_specs=[any_spec] * 2,
        out_specs=any_spec,
        scratch_shapes=[
            pltpu.VMEM((5, 4, BLK), i32),
            pltpu.VMEM((SB, BLK, BLK), bf16),
            pltpu.VMEM((1, BLK), i32),
            pltpu.SMEM((1, BLK), i32),
            pltpu.SemaphoreType.DMA((12,)),
        ],
        name="union",
        cost_estimate=cost(1_000_000),
    )(sids, src)


def call_plan(n, sids, tids, src):
    table = jax.ShapeDtypeStruct((8, BLK), i32)
    return pl.pallas_call(
        functools.partial(plan_kernel, n),
        out_shape=[blocks(c) for c in (PART, FAR, REST, CS, TAIL)] + [table] * 2,
        in_specs=[any_spec, any_spec, vm_spec],
        out_specs=[vm_spec] * 7,
        scratch_shapes=index_scratch(*[pltpu.VMEM((5, 4, BLK), i32)] * 2),
        name="plan",
        compiler_params=limit(16),
        cost_estimate=cost(500_000_000),
    )(sids, tids, src)


def call_excess(ids):
    return pl.pallas_call(
        excess_kernel,
        out_shape=jax.ShapeDtypeStruct((8, BLK), i32),
        in_specs=[vm_spec],
        out_specs=vm_spec,
        name="excess",
        compiler_params=limit(4),
        cost_estimate=cost(500_000_000),
    )(ids)


def products(plan, cls, w, tab, acc):
    first = plan[HEADS, cls]

    def step(g, carry):
        parts = []
        slots = []
        for u in range(GROUP):
            at = first + g * GROUP + u
            entry = plan[at >> 7, at & 127]
            slots.append(entry >> 16)
            parts.append(jnp.dot(w[entry & 511], tab[(entry >> 9) & 127], preferred_element_type=f32))
        for u in range(GROUP):
            acc[slots[u]] = acc[slots[u]] + parts[u]
        return carry

    lax.fori_loop(0, plan[HEADS, 16 + cls], step, 0)


def first_kernel(plan, w_hbm, src, acc, w, sems):
    step = WB // CHUNKS
    loads = []
    for i in range(CHUNKS):
        at = pl.ds(i * step, step)
        loads.append(pltpu.make_async_copy(w_hbm.at[at], w.at[at], sems.at[i]))
        loads[i].start()

    def clear(i, carry):
        acc[i] = jnp.zeros((BLK, BLK), f32)
        return carry

    lax.fori_loop(0, SLOTS, clear, 0)
    for x in loads:
        x.wait()
    products(plan, 0, w, src, acc)


acc_shape = jax.ShapeDtypeStruct((SLOTS, BLK, BLK), f32)


def call_first(plan, w, src):
    return pl.pallas_call(
        first_kernel,
        out_shape=[acc_shape, blocks(WB)],
        in_specs=[sm_spec, any_spec, vm_spec],
        out_specs=[vm_spec, vm_spec],
        scratch_shapes=[pltpu.SemaphoreType.DMA((CHUNKS,))],
        name="own",
        compiler_params=limit(24),
        cost_estimate=cost(2_000_000_000),
    )(plan, w, src)


def more_kernel(classes, plan, w, *refs):
    acc = refs[-1]
    for cls, tab in zip(classes, refs):
        products(plan, cls, w, tab, acc)


def call_more(classes, plan, w, tables, acc):
    return pl.pallas_call(
        functools.partial(more_kernel, classes),
        out_shape=acc_shape,
        in_specs=[sm_spec] + [vm_spec] * (2 + len(tables)),
        out_specs=vm_spec,
        input_output_aliases={2 + len(tables): 0},
        compiler_params=limit(VLIM),
        cost_estimate=cost(1_000_000_000),
    )(plan, w, *tables, acc)


def exchange_kernel(n, ny, acc, got, qbuf, send_sem, recv_sem):
    me = lax.axis_index(AXES)
    side = 1 - 2 * (me % 2)
    barrier = pltpu.get_barrier_semaphore()
    peers = [me + 2 * side, me - 2 * side, me - side, me + side]
    valid = [(p >= 0) & (p < n) for p in peers]
    count = 0
    for p, ok in zip(peers, valid):
        count = count + ok.astype(i32)

        @pl.when(ok)
        def _(p=p):
            pl.semaphore_signal(barrier, inc=1, device_id=(p // ny, p % ny), device_id_type=pl.DeviceIdType.MESH)

    half = CT // 2
    slots = (1, 2, 4, 3)
    comes = [valid[1], valid[0], valid[2], valid[3]]

    def quantize(c):
        f, h = c // 2, c % 2

        def four(g, carry):
            for u in range(4):
                s = g * 4 + u
                x = acc[slots[f] * CT + h * half + s]
                top = jnp.max(jnp.abs(x), axis=0, keepdims=True)
                e = jnp.ceil(jnp.log2(jnp.maximum(top, 1e-30)))
                q = jnp.clip(jnp.round(x * jnp.exp2(15.0 - e)), -32767.0, 32767.0)
                row = pl.multiple_of(s * BLK, BLK)
                qbuf[c, pl.ds(row, BLK), :] = q.astype(i32).astype(jnp.int16)
                carry = jnp.where(lax.broadcasted_iota(i32, (16, BLK), 0) == s, e.astype(i32), carry)
            return carry

        exps = lax.fori_loop(0, half // 4, four, jnp.zeros((16, BLK), i32))
        qbuf[c, pl.ds(half * BLK, 16), :] = exps.astype(jnp.int16)

    def copy(c):
        p = peers[c // 2]
        return pltpu.make_async_remote_copy(
            src_ref=qbuf.at[c],
            dst_ref=got.at[c],
            send_sem=send_sem.at[c],
            recv_sem=recv_sem.at[c],
            device_id=(p // ny, p % ny),
            device_id_type=pl.DeviceIdType.MESH,
        )

    def send(c):
        @pl.when(valid[c // 2])
        def _():
            copy(c).start()

    quantize(0)
    quantize(1)
    pl.semaphore_wait(barrier, count)
    for c in range(1, 8):
        if c > 1:
            quantize(c)
        send(c - 1)
    send(7)

    for c in range(8):

        @pl.when(valid[c // 2])
        def _(c=c):
            copy(c).wait_send()

        @pl.when(comes[c // 2])
        def _(c=c):
            copy(c).wait_recv()


def call_exchange(n, ny, acc):
    shape = (8, HALF_ROWS, BLK)
    return pl.pallas_call(
        functools.partial(exchange_kernel, n, ny),
        out_shape=jax.ShapeDtypeStruct(shape, jnp.int16),
        in_specs=[vm_spec],
        out_specs=vm_spec,
        scratch_shapes=[
            pltpu.VMEM(shape, jnp.int16),
            pltpu.SemaphoreType.DMA((8,)),
            pltpu.SemaphoreType.DMA((8,)),
        ],
        name="exchange",
        compiler_params=pltpu.CompilerParams(vmem_limit_bytes=VLIM * 1024 * 1024, collective_id=0, has_side_effects=True),
        cost_estimate=cost(1_000_000_000),
    )(acc)


def final_kernel(recv, own, got, out, total, stage, sems):
    def clear(i, carry):
        total[i] = jnp.zeros((BLK, BLK), f32)
        return carry

    lax.fori_loop(0, TB, clear, 0)

    def add_own(r, carry):
        total[recv[0, r]] = own[r]
        return carry

    lax.fori_loop(0, CT, add_own, 0)
    half = CT // 2
    for c in range(8):
        scale = jnp.exp2(got[c, pl.ds(half * BLK, 16), :].astype(f32) - 15.0)
        for r in range(half):
            t = recv[(1, 2, 4, 3)[c // 2], (c % 2) * half + r]
            total[t] = total[t] + got[c, pl.ds(r * BLK, BLK), :].astype(f32) * scale[r : r + 1, :]
    step = TB // 4
    writes = []
    for j in range(4):

        def store(i, carry):
            stage[i] = total[i].astype(bf16)
            return carry

        lax.fori_loop(j * step, (j + 1) * step, store, 0)
        at = pl.ds(j * step, step)
        writes.append(pltpu.make_async_copy(stage.at[at], out.at[at], sems.at[j]))
        if j:
            writes[j - 1].start()
    writes[3].start()
    for x in writes:
        x.wait()


def call_final(recv, own, got):
    return pl.pallas_call(
        final_kernel,
        out_shape=jax.ShapeDtypeStruct((TB, BLK, BLK), bf16),
        in_specs=[sm_spec, vm_spec, vm_spec],
        out_specs=any_spec,
        scratch_shapes=[
            pltpu.VMEM((TB + 1, BLK, BLK), f32),
            pltpu.VMEM((TB, BLK, BLK), bf16),
            pltpu.SemaphoreType.DMA((4,)),
        ],
        name="final",
        compiler_params=limit(VLIM),
        cost_estimate=cost(100_000_000),
    )(recv, own, got)


def swaps(n):
    def pairs(step):
        moves = [(d, d + step * (1 - 2 * (d % 2))) for d in range(n)]
        return [(d, t) for d, t in moves if 0 <= t < n]

    return pairs(2), pairs(-2), pairs(-1), pairs(1)


def remap(source_field, weight_blocks, source_ids, target_ids):
    n = lax.axis_size(AXES)
    out_two, in_two, across, partner = swaps(n)
    sids = source_ids.reshape(n, 4, BLK)
    tids = target_ids.reshape(n, 4, BLK)
    send = lambda x, pairs: lax.ppermute(x, AXES, pairs)
    pn = call_union(n, sids, source_field)
    got_n = send(pn, across)
    py, px, pz, pd, pt, plan, recv = call_plan(n, sids, tids, source_field)
    got_y = send(py, in_two)
    got_d = send(pd, partner)
    over = call_excess(sids)[0, 0] > 0
    tail_n, tail_y = lax.cond(
        over,
        lambda t: (send(t, across), send(t, in_two)),
        lambda t: (jnp.zeros_like(t), jnp.zeros_like(t)),
        pt,
    )
    plan, tail_n, tail_y = lax.optimization_barrier((plan, tail_n, tail_y))
    acc, w = call_first(plan, weight_blocks, source_field)
    px, pz, acc = lax.optimization_barrier((px, pz, acc))
    got_x = send(px, out_two)
    got_z = send(pz, out_two)
    swap_n = send(got_n, partner)
    acc = call_more((3, 1, 2), plan, w, (got_d, got_n, swap_n), acc)
    acc, got_y = lax.optimization_barrier((acc, got_y))
    swap_y = send(got_y, partner)
    acc = call_more((4, 5, 7, 8), plan, w, (got_y, swap_y, tail_n, tail_y), acc)
    acc = call_more((6,), plan, w, (got_x,), acc)
    acc = call_more((9,), plan, w, (got_z,), acc)
    got = call_exchange(n, lax.axis_size("gy"), acc)
    return call_final(recv, acc, got)


def solution(mesh):
    return jax.shard_map(
        remap,
        mesh=mesh,
        in_specs=(P(AXES, None, None), P(AXES, None, None), P(), P()),
        out_specs=P(AXES, None, None),
        check_vma=False,
    )
```
